256 devices in a mesh: group: 2 (over z), dp: 16 (over y, core), tensor: 8 (over x).
Axes of the slice: x: 8, y: 8, z: 2, core: 2. Of those that a mesh axis runs over, the one named last changes fastest.
The devices are a block of a 8x8x16 slice.
Arguments:
- tokens: bfloat16 [4096, 5120], P(('group', 'dp'), 'tensor'), parts along dimension 0, may hold values from -6 to 6
- router: bfloat16 [5120, 8], replicated, may hold values from -0.078125 to 0.078125
- expert_gate: bfloat16 [5120, 32768], P(None, ('dp', 'tensor')), may hold values from -0.078125 to 0.078125
- expert_up: bfloat16 [5120, 32768], P(None, ('dp', 'tensor')), may hold values from -0.078125 to 0.078125
- expert_down: bfloat16 [32768, 5120], P(('dp', 'tensor')), may hold values from -0.09375 to 0.09375
- shared_gate: bfloat16 [5120, 4096], P('dp', 'tensor'), may hold values from -0.078125 to 0.078125
- shared_up: bfloat16 [5120, 4096], P('dp', 'tensor'), may hold values from -0.078125 to 0.078125
- shared_down: bfloat16 [4096, 5120], P('tensor', 'dp'), may hold values from -0.09375 to 0.09375
- expert_ids: int32 [4096], P(('group', 'dp')), parts along dimension 0, may hold values from 0 to 7, as said below
- expert_slots: int32 [4096], P(('group', 'dp')), parts along dimension 0, may hold values from 0 to 31, as said below
Outputs:
- mixed: bfloat16 [4096, 5120], P(('group', 'dp'), 'tensor'), parts along dimension 0
The draws below stay inside these ranges and needn't reach their ends.
There are 2 independent parts, one for each index of `group`. The reference program is written for one: setup_inputs(seed, part) draws one part's arguments, and reference() takes and returns one part's arrays. A program takes and returns all parts, laid end to end along the dimension named above; an argument that names none is the same for every part. Nothing has to cross between parts.
Inputs may be any that keep to these rules, and one draw needn't show every extreme that they name: `expert_ids`: among the tokens of one index of dp no expert has more than 32; in every draw one expert has exactly 32 tokens from every index of dp. `expert_slots`: tokens of one index of dp with the same expert have distinct slots.
All inputs are finite; a program needn't handle non-finite values.
Results may differ from the reference program's by a relative error of at most 0.015.
Values may be sent and summed in bfloat16 or wider, within the bound.
No kernel may reach another device: no remote copies, remote signals or barrier semaphores. Data moves between devices by JAX's collectives and lax.ppermute only.
A program may use at most 128 MiB of HBM per device.

```python
import jax
import jax.numpy as jnp
from jax import lax

D = 5120
FFE = 4096
FFS = 4096
TOK_DEV = 128
EXPERTS = 8
CAP = 32
TOKENS = 2048
N_DP = 16
N_TENSOR = 8


def routing_pairs(key):
    base = jax.random.fold_in(key, 101)
    busiest = jax.random.randint(jax.random.fold_in(base, 1), (), 0, EXPERTS)
    block_count = TOKENS // TOK_DEV
    pair_count = EXPERTS * CAP

    def one_block(block_key):
        rank_key, jitter_key, placing_key = jax.random.split(block_key, 3)
        pair_index = jnp.arange(pair_count, dtype=jnp.int32)
        expert = pair_index // CAP
        ranking = jax.random.permutation(rank_key, EXPERTS).astype(jnp.int32)
        jitter = jax.random.randint(jitter_key, (pair_count,), 0, 4096)
        scores = jitter + ranking[expert] * 512 + jnp.where(expert == busiest, 65536, 0)
        scores = scores * pair_count + pair_index
        chosen = lax.top_k(scores, TOK_DEV)[1].astype(jnp.int32)
        placing = jax.random.permutation(placing_key, TOK_DEV)
        expert_of = jnp.zeros((TOK_DEV,), jnp.int32).at[placing].set(chosen // CAP)
        slot_of = jnp.zeros((TOK_DEV,), jnp.int32).at[placing].set(chosen % CAP)
        return (expert_of, slot_of)
    block_keys = jax.random.split(jax.random.fold_in(base, 2), block_count)
    expert_of, slot_of = jax.vmap(one_block)(block_keys)
    return (expert_of.reshape(TOKENS), slot_of.reshape(TOKENS))


def draw_expert_ids(key, part):
    return routing_pairs(key)[0]


def draw_expert_slots(key, part):
    return routing_pairs(key)[1]


def levels(rng, extent, shards, low, high):
    def one(axis_at, parts):
        draws = jax.random.uniform(jax.random.fold_in(jax.random.fold_in(rng, 6), axis_at), (parts,), jnp.float32, low / len(shards), high / len(shards))
        return jnp.repeat(jnp.exp(draws), extent[axis_at] // parts).reshape((-1,) + (1,) * (len(extent) - axis_at - 1))

    factor_of = one(*shards[0])
    for cut in shards[1:]:
        factor_of = factor_of * one(*cut)
    return factor_of


def gaussian(rng, dims, deviation, limit, cuts=(), held_as=jnp.bfloat16):
    result = jax.random.normal(rng, dims, jnp.float32) * deviation
    if len(cuts) > 0:
        result = levels(rng, dims, cuts, -0.22, 0.18) * result
    return jnp.clip(result, min=-limit, max=limit).astype(held_as)


def setup_inputs(seed: int = 0, part: int = 0) -> dict:
    splits = jax.random.split(jax.random.key(seed), 11)
    part_splits = jax.random.split(jax.random.fold_in(splits[10], part), 11)
    return {
        "tokens": gaussian(part_splits[0], (TOKENS, D), 1.0, 6.0, ((0, 16), (1, 8))),
        "router": gaussian(splits[1], (D, EXPERTS), D ** -0.5, 0.078125),
        "expert_gate": gaussian(splits[2], (D, EXPERTS * FFE), D ** -0.5, 0.078125, ((1, 128),)),
        "expert_up": gaussian(splits[3], (D, EXPERTS * FFE), D ** -0.5, 0.078125, ((1, 128),)),
        "expert_down": gaussian(splits[4], (EXPERTS * FFE, D), FFE ** -0.5, 0.09375, ((0, 128),)),
        "shared_gate": gaussian(splits[5], (D, FFS), D ** -0.5, 0.078125, ((0, 16), (1, 8))),
        "shared_up": gaussian(splits[6], (D, FFS), D ** -0.5, 0.078125, ((0, 16), (1, 8))),
        "shared_down": gaussian(splits[7], (FFS, D), FFS ** -0.5, 0.09375, ((0, 8), (1, 16))),
        "expert_ids": draw_expert_ids(jax.random.fold_in(jax.random.fold_in(splits[10], part), 71), part),
        "expert_slots": draw_expert_slots(jax.random.fold_in(jax.random.fold_in(splits[10], part), 71), part),
    }


def rounded_blocks(hidden, weight, block_count):
    row_count = hidden.shape[0]
    block_width = hidden.shape[1] // block_count
    hidden_blocks = hidden.reshape(row_count, block_count, block_width).transpose(1, 0, 2)
    weight_blocks = weight.reshape(block_count, block_width, weight.shape[1])

    def accumulate(running, inputs):
        portion = jnp.dot(inputs[0], inputs[1], preferred_element_type=jnp.float32).astype(jnp.bfloat16)
        portion = lax.optimization_barrier(portion)
        return running + portion.astype(jnp.float32), None

    running, _ = lax.scan(accumulate, jnp.zeros((row_count, weight.shape[1]), jnp.float32), (hidden_blocks, weight_blocks))
    return running


def reference(tokens, router, expert_gate, expert_up, expert_down, shared_gate, shared_up, shared_down, expert_ids, expert_slots):
    logits = jnp.dot(tokens, router, preferred_element_type=jnp.float32)
    one_hot = (expert_ids[:, None] == jnp.arange(EXPERTS, dtype=jnp.int32)[None, :]).astype(jnp.float32)
    gating = jax.nn.sigmoid(jnp.sum(logits * one_hot, axis=1))
    routed = (tokens.astype(jnp.float32) * gating[:, None]).astype(jnp.bfloat16)
    source_index = (jnp.arange(TOKENS, dtype=jnp.int32) // TOK_DEV).astype(jnp.int32)
    slot_row = (source_index * CAP + expert_slots).astype(jnp.int32)
    slot_table = jnp.zeros((EXPERTS, N_DP * CAP, D), jnp.bfloat16).at[expert_ids, slot_row].set(routed)
    gate_stack = expert_gate.reshape(D, EXPERTS, FFE).transpose(1, 0, 2)
    up_stack = expert_up.reshape(D, EXPERTS, FFE).transpose(1, 0, 2)
    down_stack = expert_down.reshape(EXPERTS, FFE, D)

    def one_expert(inputs):
        table, gate_w, up_w, down_w = inputs
        gate_sum = jnp.dot(table, gate_w, preferred_element_type=jnp.float32)
        up_sum = jnp.dot(table, up_w, preferred_element_type=jnp.float32)
        expert_hidden = (jax.nn.silu(gate_sum) * up_sum).astype(jnp.bfloat16)
        return rounded_blocks(expert_hidden, down_w, 2 * N_TENSOR).astype(jnp.bfloat16)

    expert_table = lax.map(one_expert, (slot_table, gate_stack, up_stack, down_stack))
    expert_out = expert_table[expert_ids, slot_row]
    shared_gate_sum = jnp.dot(tokens, shared_gate, preferred_element_type=jnp.float32)
    shared_up_sum = jnp.dot(tokens, shared_up, preferred_element_type=jnp.float32)
    shared_hidden = (jax.nn.silu(shared_gate_sum) * shared_up_sum).astype(jnp.bfloat16)
    shared_out = rounded_blocks(shared_hidden, shared_down, N_TENSOR)
    return (shared_out + expert_out.astype(jnp.float32)).astype(jnp.bfloat16)
```

```python
import jax
import jax.numpy as jnp
from jax import lax
from jax.sharding import PartitionSpec as P

BF = jnp.bfloat16
F32 = jnp.float32


def shift(value, axis, by):
    n = lax.axis_size(axis)
    return lax.ppermute(value, axis, [(i, (i + by) % n) for i in range(n)])


def partner(value):
    n = lax.axis_size("dp")
    return lax.ppermute(value, "dp", [(i, i ^ 1) for i in range(n)])


def ring_gather(x, axis):
    n = lax.axis_size(axis)
    half = n // 2
    rows = x.shape[0]
    blocks = {0: x}
    right, left = x, x
    for s in range(1, half):
        right = shift(right, axis, 1)
        left = shift(left, axis, -1)
        blocks[n - s] = right
        blocks[s] = left
    top = shift(right[: rows // 2], axis, 1)
    bottom = shift(left[rows // 2 :], axis, -1)
    blocks[half] = jnp.concatenate([top, bottom], axis=0)
    return blocks


def ring_scatter(term, axis, rows):
    n = lax.axis_size(axis)
    half = n // 2
    far = term(half)
    right = shift(far[: rows // 2].astype(BF), axis, 1)
    left = shift(far[rows // 2 :].astype(BF), axis, -1)
    for s in range(half - 1, 0, -1):
        own_r, own_l = term(s), term(n - s)
        if s == half - 1:
            own_r = jnp.concatenate(
                [own_r[: rows // 2] + right.astype(F32), own_r[rows // 2 :]], axis=0
            )
            own_l = jnp.concatenate(
                [own_l[: rows // 2], own_l[rows // 2 :] + left.astype(F32)], axis=0
            )
        else:
            own_r = own_r + right.astype(F32)
            own_l = own_l + left.astype(F32)
        right = shift(own_r.astype(BF), axis, 1)
        left = shift(own_l.astype(BF), axis, -1)
    return term(0) + right.astype(F32) + left.astype(F32)


def dot(a, b):
    return jnp.dot(a, b, preferred_element_type=F32)


def dot_t(a, b):
    return lax.dot_general(a, b, (((1,), (1,)), ((), ())), preferred_element_type=F32)


def on_device(
    tokens,
    router,
    expert_gate,
    expert_up,
    expert_down,
    shared_gate,
    shared_up,
    shared_down,
    expert_ids,
    expert_slots,
):
    tok_rows, width = tokens.shape
    dp_count = lax.axis_size("dp")
    n_x = lax.axis_size("tensor")
    experts = dp_count // 2
    capacity = min(2 * tok_rows // experts, tok_rows // 2)
    slots = experts * capacity
    me_y = lax.axis_index("dp") // 2
    me_x = lax.axis_index("tensor")

    def at(k):
        return lax.rem(me_x + k, n_x) * width

    both = lax.all_gather(
        jnp.concatenate([shared_gate, shared_up], axis=1), "dp", axis=0, tiled=True
    )
    down_t = lax.all_gather(shared_down.T, "dp", axis=0, tiled=True)
    gate_2, up_2, down_2 = partner(expert_gate), partner(expert_up), partner(expert_down)

    place = lax.rem(expert_ids - me_y + experts, experts) * capacity + expert_slots
    pick = (place[:, None] == jnp.arange(slots, dtype=jnp.int32)[None, :]).astype(BF)
    outgoing = lax.dot_general(
        pick, tokens, (((0,), (0,)), ((), ())), preferred_element_type=F32
    ).astype(BF)
    arrived = [outgoing[:capacity]] + [
        shift(outgoing[k * capacity : (k + 1) * capacity], "dp", 2 * k)
        for k in range(1, experts)
    ]
    served = jnp.concatenate(arrived, axis=0)

    full = jnp.zeros((tok_rows, n_x * width), BF)
    for k, block in ring_gather(tokens, "tensor").items():
        full = lax.dynamic_update_slice(full, block, (0, at(k)))

    sums = [0.0] * 5
    for k, block in ring_gather(served, "tensor").items():
        for j, w in enumerate((expert_gate, gate_2, expert_up, up_2, router)):
            rows = lax.dynamic_slice_in_dim(w, at(k), width, axis=0)
            sums[j] = sums[j] + dot(block, rows)
    chosen = (jnp.arange(experts, dtype=jnp.int32) == me_y).astype(F32)
    gating = jax.nn.sigmoid(jnp.sum(sums[4] * chosen[None, :], axis=1, keepdims=True))
    hidden_1 = (jax.nn.silu(sums[0] * gating) * (sums[2] * gating)).astype(BF)
    hidden_2 = (jax.nn.silu(sums[1] * gating) * (sums[3] * gating)).astype(BF)

    def expert_term(k):
        cols_1 = lax.dynamic_slice_in_dim(expert_down, at(k), width, axis=1)
        cols_2 = lax.dynamic_slice_in_dim(down_2, at(k), width, axis=1)
        return dot(hidden_1, cols_1) + dot(hidden_2, cols_2)

    result = ring_scatter(expert_term, "tensor", slots).astype(BF)

    back = [result[:capacity]] + [
        shift(result[k * capacity : (k + 1) * capacity], "dp", -2 * k)
        for k in range(1, experts)
    ]
    expert_out = dot(pick, jnp.concatenate(back, axis=0))

    hidden_cols = shared_gate.shape[1]
    gate_sum = dot(full, both[:, :hidden_cols])
    up_sum = dot(full, both[:, hidden_cols:])
    shared_hidden = (jax.nn.silu(gate_sum) * up_sum).astype(BF)

    def shared_term(k):
        return dot_t(shared_hidden, lax.dynamic_slice_in_dim(down_t, at(k), width, axis=0))

    shared_out = ring_scatter(shared_term, "tensor", tok_rows)
    return (shared_out + expert_out).astype(BF)


def solution(mesh):
    in_specs = (
        P(("group", "dp"), "tensor"),
        P(),
        P(None, ("dp", "tensor")),
        P(None, ("dp", "tensor")),
        P(("dp", "tensor"), None),
        P("dp", "tensor"),
        P("dp", "tensor"),
        P("tensor", "dp"),
        P(("group", "dp")),
        P(("group", "dp")),
    )
    out_specs = P(("group", "dp"), "tensor")
    return jax.shard_map(
        on_device, mesh=mesh, in_specs=in_specs, out_specs=out_specs, check_vma=False
    )
```

```python
import functools

import jax
import jax.numpy as jnp
from jax import lax
from jax.experimental import pallas as pl
from jax.experimental.pallas import tpu as pltpu
from jax.sharding import PartitionSpec as P

BF = jnp.bfloat16
F32 = jnp.float32
VMEM = pltpu.VMEM
WHOLE = pl.BlockSpec(memory_space=pltpu.VMEM)
SCALAR = pl.BlockSpec(memory_space=pltpu.SMEM)


def shift(value, axis, by):
    n = lax.axis_size(axis)
    return lax.ppermute(value, axis, [(i, (i + by) % n) for i in range(n)])


def partner(value):
    n = lax.axis_size("dp")
    return lax.ppermute(value, "dp", [(i, i ^ 1) for i in range(n)])


def ring_gather(x, axis):
    n = lax.axis_size(axis)
    half = n // 2
    rows = x.shape[0]
    ahead, behind = [], []
    right, left = x, x
    for _ in range(1, half):
        right = shift(right, axis, 1)
        left = shift(left, axis, -1)
        behind.append(right)
        ahead.append(left)
    top = shift(right[: rows // 2], axis, 1)
    bottom = shift(left[rows // 2 :], axis, -1)
    return [x, *ahead, top, bottom, *behind[::-1]]


def ring_scatter(terms, axis, late=None):
    n = lax.axis_size(axis)
    half = n // 2
    rows = terms.shape[1]
    right = shift(terms[half, : rows // 2], axis, 1)
    left = shift(terms[half, rows // 2 :], axis, -1)
    for s in range(half - 1, 0, -1):
        if s == 1 and late is not None:
            right, left, late = lax.optimization_barrier((right, left, late))
        else:
            right, left = lax.optimization_barrier((right, left))
        own_r, own_l = terms[s], terms[n - s]
        if s == half - 1:
            pad_r = jnp.pad(right, ((0, rows // 2), (0, 0)))
            pad_l = jnp.pad(left, ((rows // 2, 0), (0, 0)))
        else:
            pad_r, pad_l = right, left
        right = shift((own_r.astype(F32) + pad_r.astype(F32)).astype(BF), axis, 1)
        left = shift((own_l.astype(F32) + pad_l.astype(F32)).astype(BF), axis, -1)
    return (terms[0], right, left), late


def dot(a, b):
    return jnp.dot(a, b, preferred_element_type=F32)


def dot_t(a, b):
    return lax.dot_general(a, b, (((1,), (1,)), ((), ())), preferred_element_type=F32)


def silu(v):
    return v / (1.0 + jnp.exp(-v))


def one_hot_rows(me_y, ids, slots, experts, capacity):
    place = lax.rem(ids - me_y + experts, experts) * capacity + slots
    rows = lax.broadcasted_iota(jnp.int32, (experts * capacity, ids.shape[1]), 0)
    return (rows == place).astype(F32).astype(BF)


def dispatch_kernel(experts, capacity, me_y, ids, slots, tokens, *outs):
    pick = one_hot_rows(me_y[0], ids[...], slots[...], experts, capacity)
    rows = dot(pick, tokens[...]).astype(BF)
    for k, out in enumerate(outs):
        out[...] = rows[k * capacity : (k + 1) * capacity]


def join_kernel(*refs):
    out = refs[-1]
    at = 0
    for ref in refs[:-1]:
        out[at : at + ref.shape[0], :] = ref[...]
        at += ref.shape[0]


def fill(held, pieces, n):
    half = n // 2
    rows = held.shape[1]
    for k in range(half):
        held[k] = pieces[k][...]
    held[half, : rows // 2, :] = pieces[half][...]
    held[half, rows // 2 :, :] = pieces[half + 1][...]
    for k in range(half + 1, n):
        held[k] = pieces[k + 1][...]


def expert_kernel(n, experts, me_x, me_y, *refs):
    pieces = refs[: n + 1]
    gate_1, gate_2, up_1, up_2, router, down_1, down_2, out = refs[n + 1 : n + 9]
    held, sums, logits, hidden = refs[n + 9 :]
    i = pl.program_id(0)
    cols = gate_1.shape[1]

    @pl.when(i == 0)
    def _():
        fill(held, pieces, n)
        sums[...] = jnp.zeros_like(sums)
        logits[...] = jnp.zeros_like(logits)

    @pl.when(i < n)
    def _():
        x = held[i]
        sums[0] += dot(x, gate_1[...])
        sums[1] += dot(x, gate_2[...])
        sums[2] += dot(x, up_1[...])
        sums[3] += dot(x, up_2[...])
        logits[...] += dot_t(x, router[...])

    @pl.when(i == n - 1)
    def _():
        mine = lax.broadcasted_iota(jnp.int32, logits.shape, 1) == me_y[0]
        logit = jnp.sum(jnp.where(mine, logits[...], 0.0), axis=1, keepdims=True)
        gating = jax.nn.sigmoid(logit)
        for h in range(2):
            act = silu(sums[h] * gating) * (sums[2 + h] * gating)
            hidden[:, h * cols : (h + 1) * cols] = act.astype(BF)

    @pl.when(i >= n)
    def _():
        out[0] = (
            dot(hidden[:, :cols], down_1[...]) + dot(hidden[:, cols:], down_2[...])
        ).astype(BF)


def shared_kernel(n, me_x, *refs):
    pieces = refs[: n + 1]
    gate_up, down_t, out, held, sums, hidden = refs[n + 1 :]
    i = pl.program_id(0)
    cols = hidden.shape[1]

    @pl.when(i == 0)
    def _():
        fill(held, pieces, n)
        sums[...] = jnp.zeros_like(sums)

    @pl.when(i < n)
    def _():
        sums[...] += dot(held[i], gate_up[...])

    @pl.when(i == n - 1)
    def _():
        hidden[...] = (silu(sums[:, :cols]) * sums[:, cols:]).astype(BF)

    @pl.when(i >= n)
    def _():
        out[0] = dot_t(hidden[...], down_t[...]).astype(BF)


def combine_kernel(experts, capacity, me_y, ids, slots, *refs):
    blocks = refs[:experts]
    shared, out, held = refs[experts : experts + 3], refs[experts + 3], refs[experts + 4]
    for k, block in enumerate(blocks):
        held[k * capacity : (k + 1) * capacity, :] = block[...]
    pick = one_hot_rows(me_y[0], ids[...], slots[...], experts, capacity)
    total = lax.dot_general(
        pick, held[...], (((0,), (0,)), ((), ())), preferred_element_type=F32
    )
    for piece in shared:
        total = total + piece[...].astype(F32)
    out[...] = total.astype(BF)


def cost(flops, read):
    return pl.CostEstimate(flops=int(flops), bytes_accessed=int(read), transcendentals=0)


def on_device(
    tokens,
    router,
    expert_gate,
    expert_up,
    expert_down,
    shared_gate,
    shared_up,
    shared_down,
    expert_ids,
    expert_slots,
):
    tok_rows, width = tokens.shape
    dp_count = lax.axis_size("dp")
    n = lax.axis_size("tensor")
    half = n // 2
    experts = dp_count // 2
    capacity = min(2 * tok_rows // experts, tok_rows // 2)
    slots = experts * capacity
    me_y = (lax.axis_index("dp") // 2).astype(jnp.int32).reshape(1)
    me_x = lax.axis_index("tensor").astype(jnp.int32).reshape(1)
    ids, places = expert_ids.reshape(1, -1), expert_slots.reshape(1, -1)
    ffs = shared_gate.shape[1]
    ffe = expert_gate.shape[1]

    weights = lax.all_gather(
        jnp.concatenate([shared_gate, shared_up, shared_down.T], axis=1), "dp", axis=0, tiled=True
    )
    gate_2, up_2, down_2 = partner(expert_gate), partner(expert_up), partner(expert_down)

    block = jax.ShapeDtypeStruct((capacity, width), BF)
    outgoing = list(pl.pallas_call(
        functools.partial(dispatch_kernel, experts, capacity),
        out_shape=[block] * experts,
        in_specs=[SCALAR, WHOLE, WHOLE, WHOLE],
        out_specs=[WHOLE] * experts,
        cost_estimate=cost(2 * slots * tok_rows * width, 1 << 19),
        name="dispatch",
        compiler_params=pltpu.CompilerParams(vmem_limit_bytes=4 << 20),
    )(me_y, ids, places, tokens))
    ring_tokens, outgoing[0] = lax.optimization_barrier((tokens, outgoing[0]))
    arrived = [outgoing[0]] + [shift(outgoing[k], "dp", 2 * k) for k in range(1, experts)]
    served = pl.pallas_call(
        join_kernel,
        out_shape=jax.ShapeDtypeStruct((slots, width), BF),
        in_specs=[WHOLE] * experts,
        out_specs=WHOLE,
        cost_estimate=cost(1 << 20, 1 << 19),
        name="join",
        compiler_params=pltpu.CompilerParams(vmem_limit_bytes=4 << 20),
    )(*arrived)

    token_pieces = ring_gather(ring_tokens, "tensor")
    served, *token_pieces[half : half + 2] = lax.optimization_barrier(
        (served, *token_pieces[half : half + 2])
    )
    slot_pieces = ring_gather(served, "tensor")

    def whole(piece):
        return pl.BlockSpec(piece.shape, lambda i, *_: (0, 0))

    def row(i, me, *_):
        return lax.rem(me[0] + jnp.minimum(i, n - 1), n)

    def late(i, me, *_):
        return lax.rem(me[0] + jnp.maximum(i - n, 0), n)

    up_spec = pl.BlockSpec((width, ffe), lambda i, me, *_: (row(i, me), 0))
    down_spec = pl.BlockSpec((ffe, width), lambda i, me, *_: (0, late(i, me)))
    expert_terms = pl.pallas_call(
        functools.partial(expert_kernel, n, experts),
        out_shape=jax.ShapeDtypeStruct((n, slots, width), BF),
        grid_spec=pltpu.PrefetchScalarGridSpec(
            num_scalar_prefetch=2,
            grid=(2 * n,),
            in_specs=[whole(p) for p in slot_pieces]
            + [up_spec] * 4
            + [
                pl.BlockSpec((experts, width), lambda i, me, *_: (0, row(i, me))),
                down_spec,
                down_spec,
            ],
            out_specs=pl.BlockSpec((1, slots, width), lambda i, *_: (jnp.maximum(i - n, 0), 0, 0)),
            scratch_shapes=[
                VMEM((n, slots, width), BF),
                VMEM((4, slots, ffe), F32),
                VMEM((slots, experts), F32),
                VMEM((slots, 2 * ffe), BF),
            ],
        ),
        cost_estimate=cost(12 * slots * n * width * ffe, 24 * n * width * ffe // 2),
        name="expert_mlp",
        compiler_params=pltpu.CompilerParams(vmem_limit_bytes=54 << 20),
    )(me_x, me_y, *slot_pieces, expert_gate, gate_2, expert_up, up_2, router.T, expert_down, down_2)

    (own, right, left), weights = ring_scatter(expert_terms, "tensor", weights)
    result = (own.astype(F32) + right.astype(F32) + left.astype(F32)).astype(BF)

    back = [result[:capacity]] + [
        shift(result[k * capacity : (k + 1) * capacity], "dp", -2 * k)
        for k in range(1, experts)
    ]

    shared_terms = pl.pallas_call(
        functools.partial(shared_kernel, n),
        out_shape=jax.ShapeDtypeStruct((n, tok_rows, width), BF),
        grid_spec=pltpu.PrefetchScalarGridSpec(
            num_scalar_prefetch=1,
            grid=(2 * n,),
            in_specs=[whole(p) for p in token_pieces]
            + [
                pl.BlockSpec((width, 2 * ffs), lambda i, me: (row(i, me), 0)),
                pl.BlockSpec((width, ffs), lambda i, me: (late(i, me), 2)),
            ],
            out_specs=pl.BlockSpec(
                (1, tok_rows, width), lambda i, *_: (jnp.maximum(i - n, 0), 0, 0)
            ),
            scratch_shapes=[
                VMEM((n, tok_rows, width), BF),
                VMEM((tok_rows, 2 * ffs), F32),
                VMEM((tok_rows, ffs), BF),
            ],
        ),
        cost_estimate=cost(6 * tok_rows * n * width * ffs, 6 * n * width * ffs),
        name="shared_mlp",
        compiler_params=pltpu.CompilerParams(vmem_limit_bytes=50 << 20),
    )(me_x, *token_pieces, weights, weights)
    shared_out, _ = ring_scatter(shared_terms, "tensor")

    return pl.pallas_call(
        functools.partial(combine_kernel, experts, capacity),
        out_shape=jax.ShapeDtypeStruct((tok_rows, width), BF),
        in_specs=[SCALAR] + [WHOLE] * (experts + 5),
        out_specs=WHOLE,
        scratch_shapes=[VMEM((slots, width), BF)],
        cost_estimate=cost(2 * slots * tok_rows * width, 1 << 20),
        name="combine",
        compiler_params=pltpu.CompilerParams(vmem_limit_bytes=4 << 20),
    )(me_y, ids, places, *back, *shared_out)


def solution(mesh):
    in_specs = (
        P(("group", "dp"), "tensor"),
        P(),
        P(None, ("dp", "tensor")),
        P(None, ("dp", "tensor")),
        P(("dp", "tensor"), None),
        P("dp", "tensor"),
        P("dp", "tensor"),
        P("tensor", "dp"),
        P(("group", "dp")),
        P(("group", "dp")),
    )
    out_specs = P(("group", "dp"), "tensor")
    return jax.shard_map(
        on_device, mesh=mesh, in_specs=in_specs, out_specs=out_specs, check_vma=False
    )
```
